32 devices in a mesh: row: 4 (over z), col: 8 (over y, x, core).
Axes of the slice: x: 2, y: 2, z: 4, core: 2. Of those that a mesh axis runs over, the one named last changes fastest.
Arguments:
- a_blocks: bfloat16 [8, 8, 43, 128, 128], P('col', 'row'), may hold values from -6 to 6
- a_index: int32 [8, 8, 43], P('col', 'row'), may hold values from 0 to 479, as said below
- b_blocks: bfloat16 [8, 8, 43, 128, 128], P('col', 'row'), may hold values from -0.5 to 0.5
- b_index: int32 [8, 8, 43], P('col', 'row'), may hold values from 0 to 479, as said below
- pair_list: int32 [8, 8, 3, 2, 40], P('col', 'row'), may hold values from 0 to 42, as said below
- pair_count: int32 [8, 8, 3], P('col', 'row'), may hold values from 0 to 40, as said below
Outputs:
- c_window: bfloat16 [10240, 10240], P('col', 'row')
The draws below stay inside these ranges and needn't reach their ends.
Inputs may be any that keep to these rules, and one draw needn't show every extreme that they name: a_index[p, k, j] = 10 * (block column) + (block row) of stored slot j in A panel (p, k); the slots of one panel hold distinct positions. b_index[k, q, j] = 10 * (block row) + (block column) of stored slot j in B panel (k, q); the slots of one panel hold distinct positions. `pair_list`: entry j < pair_count[p, q, s] of list (p, q, s) names a slot a of A panel (p, k) and a slot b of B panel (k, q), k = (p + q + s) mod 8, with a_index // 10 equal to b_index // 10; no pair twice in a list; entries from pair_count on are zero. `pair_count`: in every draw some list is full.
All inputs are finite; a program needn't handle non-finite values.
Results may differ from the reference program's by a relative error of at most 0.001.
Values may be sent and summed in bfloat16 or wider, within the bound.
No kernel may reach another device: no remote copies, remote signals or barrier semaphores. Data moves between devices by JAX's collectives and lax.ppermute only.
A program may use at most 128 MiB of HBM per device.

```python
import jax
import jax.numpy as jnp
from jax import lax

BS = 128
KB = 48
WB = 10
STEPS = 3
PANELS = 8
CAP = 43
PAIRS = 40


def panel_ids(key, forced):
    slots = WB * KB
    spread = jax.random.permutation(key, slots).astype(jnp.int32)
    rest = jax.random.permutation(jax.random.fold_in(key, 3), slots - WB).astype(jnp.int32)
    leading = jnp.concatenate([jnp.arange(WB, dtype=jnp.int32), WB + rest])
    return jnp.where(forced, leading, spread)[:CAP]


def occupancy(key):
    base = jax.random.fold_in(key, 11)
    keys = jax.random.split(base, 8)
    row_pick = jax.random.randint(keys[0], (), 0, PANELS)
    col_pick = jax.random.randint(keys[1], (), 0, PANELS)
    inner_pick = (row_pick + col_pick) % PANELS
    first_axis = jnp.arange(PANELS)[:, None]
    second_axis = jnp.arange(PANELS)[None, :]
    forced_a = ((first_axis == row_pick) & (second_axis == inner_pick)).reshape(-1)
    forced_b = ((first_axis == inner_pick) & (second_axis == col_pick)).reshape(-1)
    a_ids = jax.vmap(panel_ids)(jax.random.split(keys[2], PANELS * PANELS), forced_a).reshape(PANELS, PANELS, CAP)
    b_ids = jax.vmap(panel_ids)(jax.random.split(keys[3], PANELS * PANELS), forced_b).reshape(PANELS, PANELS, CAP)
    flat_panels = jnp.arange(PANELS * PANELS).reshape(PANELS, PANELS)
    a_live = jax.random.randint(keys[4], (PANELS, PANELS), CAP // 2, CAP + 1)
    a_full = jax.random.randint(keys[5], (), 0, PANELS * PANELS)
    a_live = jnp.where(flat_panels == a_full, CAP, a_live)
    b_live = jax.random.randint(keys[6], (PANELS, PANELS), CAP // 2, CAP + 1)
    b_full = jax.random.randint(keys[7], (), 0, PANELS * PANELS)
    b_live = jnp.where(flat_panels == b_full, CAP, b_live)
    return (a_ids, a_live, b_ids, b_live)


def pair_tables(key):
    a_ids, a_live, b_ids, b_live = occupancy(key)

    def one_list(row_panel, col_panel, step_no):
        inner = (row_panel + col_panel + step_no) % PANELS
        slot_range = jnp.arange(CAP)
        a_inner = a_ids[row_panel, inner] // WB
        b_inner = b_ids[inner, col_panel] // WB
        matched = (slot_range[:, None] < a_live[row_panel, inner]) & (slot_range[None, :] < b_live[inner, col_panel]) & (a_inner[:, None] == b_inner[None, :])
        flat_pos = jnp.arange(CAP * CAP)
        ranked = jnp.sort(jnp.where(matched.reshape(-1), flat_pos, CAP * CAP + flat_pos))[:PAIRS]
        live_count = jnp.minimum(jnp.sum(matched.astype(jnp.int32)), PAIRS)
        is_live = jnp.arange(PAIRS) < live_count
        a_slots = jnp.where(is_live, ranked // CAP, 0)
        b_slots = jnp.where(is_live, ranked % CAP, 0)
        return (jnp.stack([a_slots, b_slots]).astype(jnp.int32), live_count.astype(jnp.int32))
    rows_grid, cols_grid, steps_grid = jnp.meshgrid(jnp.arange(PANELS), jnp.arange(PANELS), jnp.arange(STEPS), indexing='ij')
    lists, counts = jax.vmap(one_list)(rows_grid.reshape(-1), cols_grid.reshape(-1), steps_grid.reshape(-1))
    return (lists.reshape(PANELS, PANELS, STEPS, 2, PAIRS), counts.reshape(PANELS, PANELS, STEPS))


def draw_a_index(key, part):
    return occupancy(key)[0].astype(jnp.int32)


def draw_b_index(key, part):
    return occupancy(key)[2].astype(jnp.int32)


def draw_pair_list(key, part):
    return pair_tables(key)[0]


def draw_pair_count(key, part):
    return pair_tables(key)[1]


def steps_of(key, extent, pieces, smallest, top_value):
    def one(axis_at, parts):
        steps = jax.random.uniform(jax.random.fold_in(jax.random.fold_in(key, 6), axis_at), (parts,), jnp.float32, smallest / len(pieces), top_value / len(pieces))
        return jnp.repeat(jnp.exp(steps), extent[axis_at] // parts).reshape((-1,) + (1,) * (len(extent) - axis_at - 1))

    level = one(*pieces[0])
    for cut in pieces[1:]:
        level = level * one(*cut)
    return level


def normal_values(own_key, shape, scale, limit, pieces=(), kind=jnp.bfloat16):
    entries = jax.random.normal(own_key, shape, jnp.float32) * scale
    if len(pieces) > 0:
        entries = steps_of(own_key, shape, pieces, -0.22, 0.18) * entries
    return jnp.clip(entries, min=-limit, max=limit).astype(kind)


def setup_inputs(seed: int = 0) -> dict:
    arg_keys = jax.random.split(jax.random.key(seed), 7)
    a_blocks = normal_values(arg_keys[0], (PANELS, PANELS, CAP, BS, BS), 1.0, 6.0, ((0, 8), (1, 4)))
    a_index = draw_a_index(jax.random.fold_in(arg_keys[6], 71), 0)
    b_blocks = normal_values(arg_keys[2], (PANELS, PANELS, CAP, BS, BS), BS ** -0.5, 0.5, ((0, 8), (1, 4)))
    b_index = draw_b_index(jax.random.fold_in(arg_keys[6], 71), 0)
    pair_list = draw_pair_list(jax.random.fold_in(arg_keys[6], 71), 0)
    pair_count = draw_pair_count(jax.random.fold_in(arg_keys[6], 71), 0)
    return dict(a_blocks=a_blocks, a_index=a_index, b_blocks=b_blocks, b_index=b_index, pair_list=pair_list, pair_count=pair_count)


def panel_product(a_blocks, a_index, b_blocks, b_index, pair_list, pair_count, row_panel, col_panel):
    panels = a_blocks.shape[0]
    edge = a_blocks.shape[-1]
    running = jnp.zeros((WB * WB, edge, edge), jnp.float32)
    for step_no in range(STEPS):
        inner = ((row_panel + col_panel + step_no) % panels).astype(jnp.int32)
        a_slots = pair_list[row_panel, col_panel, step_no, 0].astype(jnp.int32)
        b_slots = pair_list[row_panel, col_panel, step_no, 1].astype(jnp.int32)
        is_live = (jnp.arange(a_slots.shape[0], dtype=jnp.int32) < pair_count[row_panel, col_panel, step_no]).astype(jnp.float32)
        lhs_blocks = a_blocks[row_panel, inner][a_slots].astype(jnp.float32)
        rhs_blocks = b_blocks[inner, col_panel][b_slots].astype(jnp.float32)
        products = jnp.einsum("pij,pjk->pik", lhs_blocks, rhs_blocks) * is_live[:, None, None]
        target = (a_index[row_panel, inner][a_slots] % WB) * WB + b_index[inner, col_panel][b_slots] % WB
        running = running + jax.ops.segment_sum(products, target.astype(jnp.int32), num_segments=WB * WB)
    grid = running.reshape(WB, WB, edge, edge).transpose(0, 2, 1, 3).reshape(WB * edge, WB * edge)
    return grid.astype(jnp.bfloat16)


def reference(a_blocks, a_index, b_blocks, b_index, pair_list, pair_count):
    panels = a_blocks.shape[0]
    columns = a_blocks.shape[1]
    edge = a_blocks.shape[-1]

    def one_row(row_panel):
        def one_col(col_panel):
            return panel_product(a_blocks, a_index, b_blocks, b_index, pair_list, pair_count, row_panel, col_panel)
        return lax.map(one_col, jnp.arange(columns, dtype=jnp.int32))

    stacked = lax.map(one_row, jnp.arange(panels, dtype=jnp.int32))
    return stacked.transpose(0, 2, 1, 3).reshape(panels * WB * edge, columns * WB * edge)
```

```python
import jax
import jax.numpy as jnp
from jax import lax
from jax.experimental import pallas as pl
from jax.experimental.pallas import tpu as pltpu
from jax.sharding import PartitionSpec as P

WB = 10
GROUP = 8


def multiply_kernel(meta, *refs):
    cap, edge = refs[0].shape[0], refs[0].shape[-1]
    out, a_buf, b_buf, acc, stage, a_sems, b_sems, out_sems = refs[-8:]
    wanted_count = a_buf.shape[0] // cap
    a_panels, b_panels = refs[:wanted_count], refs[wanted_count:-8]
    lists = len(b_panels)

    def a_copy(w):
        return pltpu.make_async_copy(a_panels[w], a_buf.at[pl.ds(w * cap, cap)], a_sems.at[w])

    def b_copy(n):
        return pltpu.make_async_copy(b_panels[n], b_buf.at[pl.ds(n * cap, cap)], b_sems.at[n])

    for w in range(wanted_count):
        a_copy(w).start()
    for n in range(lists):
        b_copy(n).start()

    def clear(t, carry):
        acc[t] = jnp.zeros((edge, edge), jnp.float32)
        return carry

    lax.fori_loop(0, acc.shape[0], clear, 0)
    for w in range(wanted_count):
        a_copy(w).wait()
    for n in range(lists):
        b_copy(n).wait()

        def group(g, carry, n=n):
            products = []
            targets = []
            for u in range(GROUP):
                j = g * GROUP + u
                lhs = a_buf[meta[n, j]]
                rhs = b_buf[meta[lists + n, j]]
                targets.append(meta[2 * lists + n, j])
                products.append(jnp.dot(lhs, rhs, preferred_element_type=jnp.float32))
            for u in range(GROUP):
                acc[targets[u]] = acc[targets[u]] + products[u]
            return carry

        lax.fori_loop(0, pl.cdiv(meta[3 * lists, n], GROUP), group, 0)

    def out_copy(r):
        rows = pl.ds(r * edge, edge)
        return pltpu.make_async_copy(stage.at[rows], out.at[rows], out_sems.at[r])

    def finish(r, carry):
        for half in range(2):
            for c in range(WB):
                block = acc[half * WB * WB + r * WB + c].astype(jnp.bfloat16)
                stage[pl.ds(r * edge, edge), (half * WB + c) * edge : (half * WB + c + 1) * edge] = block
        out_copy(r).start()
        return carry

    lax.fori_loop(0, WB, finish, 0)
    for r in range(WB):
        out_copy(r).wait()


def body(a_blocks, a_index, b_blocks, b_index, pair_list, pair_count):
    cap, edge = a_blocks.shape[2], a_blocks.shape[-1]
    steps, pair_cap = pair_list.shape[2], pair_list.shape[-1]
    cols, rows = lax.axis_size("col"), lax.axis_size("row")
    column = lax.axis_index("col")
    row_index = lax.axis_index("row")
    core = column % 2
    half_common = (steps - 1) // 2

    fetched, mids, swapped = [], [], []
    for slot in range(2):
        shared = list(range(slot + 1, slot + steps))
        offsets = (
            [slot] + shared[:half_common],
            [slot + steps] + shared[half_common:][::-1],
        )
        got = [None] * (half_common + 1)
        for j in list(range(1, half_common + 1)) + [0]:
            moves = []
            for i in range(cols):
                for r in range(rows):
                    source = (i // 2 * 2 + 2 * r + offsets[i % 2][j]) % cols
                    moves.append((r * cols + source, r * cols + i))
            got[j] = lax.ppermute(b_blocks[0, slot], ("row", "col"), moves)
        fetched.append(got)
        across = [(i, i ^ 1) for i in range(cols)]
        swapped.append([lax.ppermute(got[j], "col", across) for j in range(1, half_common + 1)])
    ordered = (lax.dynamic_index_in_dim(a_blocks[0], core, 0, False), lax.dynamic_index_in_dim(a_blocks[0], 1 - core, 0, False))
    a_panels = []
    for w in range(steps + 1):
        moves = []
        for i in range(cols):
            for r in range(rows):
                source = (i + 2 * r + w) % cols // 2
                moves.append((source * cols + i, r * cols + i))
        a_panels.append(lax.ppermute(ordered[w % 2], ("row", "col"), moves))

    ids = jnp.concatenate([a_index[0], b_index[0]], axis=-1)
    all_ids = lax.all_gather(ids, ("row", "col"), axis=0).reshape(rows, cols, 2, 2, cap)
    all_ids = all_ids.transpose(1, 0, 2, 3, 4).reshape(cols, 2 * rows, 2, cap)

    pairs = jnp.where(core == 0, pair_list[0], pair_list[0][:, ::-1])
    counts = jnp.where(core == 0, pair_count[0], pair_count[0][:, ::-1])
    place = jnp.arange(steps)
    step = jnp.where(core == 0, place, steps - 1 - place)
    half = jnp.arange(2)
    inner = (column + 2 * row_index + half[:, None] + step[None, :]) % cols
    a_slots, b_slots = pairs[:, :, 0], pairs[:, :, 1]
    a_ids = all_ids[column][inner][:, :, 0]
    b_ids = all_ids[inner, 2 * row_index + half[:, None]][:, :, 1]
    a_at = jnp.take_along_axis(a_ids, a_slots, axis=-1) % WB
    b_at = jnp.take_along_axis(b_ids, b_slots, axis=-1) % WB
    live = jnp.arange(pair_cap) < counts[:, :, None]
    target = jnp.where(live, half[:, None, None] * (WB * WB) + a_at * WB + b_at, 2 * WB * WB)
    a_slots = a_slots + (half[:, None] + step[None, :])[:, :, None] * cap
    b_slots = b_slots + (half[:, None] * steps + place[None, :])[:, :, None] * cap
    lists = 2 * steps
    padded = -(-max(pair_cap, lists) // GROUP) * GROUP

    def laid(x, fill=0):
        x = x.reshape(-1, x.shape[-1]).astype(jnp.int32)
        return jnp.pad(x, ((0, 0), (0, padded - x.shape[1])), constant_values=fill)

    meta = jnp.concatenate(
        [laid(a_slots), laid(b_slots), laid(target, 2 * WB * WB), laid(counts.reshape(1, lists))]
    )

    panels = []
    for slot in range(2):
        panels += fetched[slot] + swapped[slot]
    any_space = pl.BlockSpec(memory_space=pl.ANY)
    return pl.pallas_call(
        multiply_kernel,
        out_shape=jax.ShapeDtypeStruct((WB * edge, 2 * WB * edge), jnp.bfloat16),
        in_specs=[pl.BlockSpec(memory_space=pltpu.SMEM)] + [any_space] * (steps + 1 + lists),
        out_specs=any_space,
        scratch_shapes=[
            pltpu.VMEM(((steps + 1) * cap, edge, edge), jnp.bfloat16),
            pltpu.VMEM((lists * cap, edge, edge), jnp.bfloat16),
            pltpu.VMEM((2 * WB * WB + 1, edge, edge), jnp.float32),
            pltpu.VMEM((WB * edge, 2 * WB * edge), jnp.bfloat16),
            pltpu.SemaphoreType.DMA((steps + 1,)),
            pltpu.SemaphoreType.DMA((lists,)),
            pltpu.SemaphoreType.DMA((WB,)),
        ],
        compiler_params=pltpu.CompilerParams(vmem_limit_bytes=48 * 1024 * 1024),
        name="pair_products",
    )(meta, *a_panels, *panels)


def solution(mesh):
    in_specs = (
        P("col", "row", None, None, None),
        P("col", "row", None),
        P("col", "row", None, None, None),
        P("col", "row", None),
        P("col", "row", None, None, None),
        P("col", "row", None),
    )
    out_specs = P("col", "row")
    return jax.shard_map(body, mesh=mesh, in_specs=in_specs, out_specs=out_specs, check_vma=False)
```

```python
import jax
import jax.numpy as jnp
from jax import lax
from jax.experimental import pallas as pl
from jax.experimental.pallas import tpu as pltpu
from jax.sharding import PartitionSpec as P

WB = 10
GROUP = 8


def multiply_kernel(meta, *refs):
    cap, edge = refs[0].shape[0], refs[0].shape[-1]
    out, a_buf, b_buf, acc, stage, a_sems, b_sems, out_sems = refs[-8:]
    wanted_count = a_buf.shape[0] // cap
    a_panels, b_panels = refs[:wanted_count], refs[wanted_count:-8]
    lists = len(b_panels)

    def a_copy(w):
        return pltpu.make_async_copy(a_panels[w], a_buf.at[pl.ds(w * cap, cap)], a_sems.at[w])

    def b_copy(n):
        return pltpu.make_async_copy(b_panels[n], b_buf.at[pl.ds(n * cap, cap)], b_sems.at[n])

    for w in range(wanted_count):
        a_copy(w).start()
    for n in range(lists):
        b_copy(n).start()

    def clear(t, carry):
        acc[t] = jnp.zeros((edge, edge), jnp.float32)
        return carry

    lax.fori_loop(0, acc.shape[0], clear, 0)
    for w in range(wanted_count):
        a_copy(w).wait()
    for n in range(lists):
        b_copy(n).wait()

        def group(g, carry, n=n):
            products = []
            targets = []
            for u in range(GROUP):
                j = g * GROUP + u
                lhs = a_buf[meta[n, j]]
                rhs = b_buf[meta[lists + n, j]]
                targets.append(meta[2 * lists + n, j])
                products.append(jnp.dot(lhs, rhs, preferred_element_type=jnp.float32))
            for u in range(GROUP):
                acc[targets[u]] = acc[targets[u]] + products[u]
            return carry

        lax.fori_loop(0, pl.cdiv(meta[3 * lists, n], GROUP), group, 0)

    def out_copy(r):
        rows = pl.ds(r * edge, edge)
        return pltpu.make_async_copy(stage.at[rows], out.at[rows], out_sems.at[r])

    def finish(r, carry):
        for half in range(2):
            for c in range(WB):
                block = acc[half * WB * WB + r * WB + c].astype(jnp.bfloat16)
                stage[pl.ds(r * edge, edge), (half * WB + c) * edge : (half * WB + c + 1) * edge] = block
        out_copy(r).start()
        return carry

    lax.fori_loop(0, WB, finish, 0)
    for r in range(WB):
        out_copy(r).wait()


def body(a_blocks, a_index, b_blocks, b_index, pair_list, pair_count):
    cap, edge = a_blocks.shape[2], a_blocks.shape[-1]
    steps, pair_cap = pair_list.shape[2], pair_list.shape[-1]
    cols, rows = lax.axis_size("col"), lax.axis_size("row")
    column = lax.axis_index("col")
    row_index = lax.axis_index("row")
    core = column % 2
    half_common = (steps - 1) // 2
    hop = steps // 2 * 2
    ordered = (
        lax.dynamic_index_in_dim(a_blocks[0], core, 0, False),
        lax.dynamic_index_in_dim(a_blocks[0], 1 - core, 0, False),
    )
    first_a, second_a = [], []
    for w in range(hop):
        moves = []
        for i in range(cols):
            for r in range(rows):
                far = w if 2 * i < cols else w + hop
                moves.append(((i + 2 * r + far) % cols // 2 * cols + i, r * cols + i))
        first_a.append(lax.ppermute(ordered[w % 2], ("row", "col"), moves))
    for w in range(hop):
        moves = []
        for i in range(cols):
            for r in range(rows):
                source = (r + (1 if 2 * i < cols else -1) * (hop // 2)) % rows
                moves.append((source * cols + i, r * cols + i))
        second_a.append(lax.ppermute(first_a[w], ("row", "col"), moves))
    a_panels = first_a + second_a

    ids = jnp.concatenate([a_index[0], b_index[0]], axis=-1)
    all_ids = lax.all_gather(ids, ("row", "col"), axis=0).reshape(rows, cols, 2, 2, cap)
    all_ids = all_ids.transpose(1, 0, 2, 3, 4).reshape(cols, 2 * rows, 2, cap)

    pairs = jnp.where(core == 0, pair_list[0], pair_list[0][:, ::-1])
    counts = jnp.where(core == 0, pair_count[0], pair_count[0][:, ::-1])
    place = jnp.arange(steps)
    step = jnp.where(core == 0, place, steps - 1 - place)
    half = jnp.arange(2)
    inner = (column + 2 * row_index + half[:, None] + step[None, :]) % cols
    a_slots, b_slots = pairs[:, :, 0], pairs[:, :, 1]
    a_ids = all_ids[column][inner][:, :, 0]
    b_ids = all_ids[inner, 2 * row_index + half[:, None]][:, :, 1]
    a_at = jnp.take_along_axis(a_ids, a_slots, axis=-1) % WB
    b_at = jnp.take_along_axis(b_ids, b_slots, axis=-1) % WB
    live = jnp.arange(pair_cap) < counts[:, :, None]
    target = jnp.where(live, half[:, None, None] * (WB * WB) + a_at * WB + b_at, 2 * WB * WB)
    a_place = (half[:, None] + step[None, :] + jnp.where(2 * column < cols, 0, hop)) % (2 * hop)
    a_slots = a_slots + a_place[:, :, None] * cap
    b_slots = b_slots + (half[:, None] * steps + place[None, :])[:, :, None] * cap
    lists = 2 * steps
    padded = -(-max(pair_cap, lists) // GROUP) * GROUP

    def laid(x, fill=0):
        x = x.reshape(-1, x.shape[-1]).astype(jnp.int32)
        return jnp.pad(x, ((0, 0), (0, padded - x.shape[1])), constant_values=fill)

    meta = jnp.concatenate(
        [laid(a_slots), laid(b_slots), laid(target, 2 * WB * WB), laid(counts.reshape(1, lists))]
    )

    fetched, swapped = [], []
    for slot in range(2):
        shared = list(range(slot + 1, slot + steps))
        offsets = (
            [slot] + shared[:half_common],
            [slot + steps] + shared[half_common:][::-1],
        )
        got = [None] * (half_common + 1)
        held, all_ids = lax.optimization_barrier((b_blocks[0, slot], all_ids))
        for j in list(range(1, half_common + 1)) + [0]:
            moves = []
            for i in range(cols):
                for r in range(rows):
                    source = (i // 2 * 2 + 2 * r + offsets[i % 2][j]) % cols
                    moves.append((r * cols + source, r * cols + i))
            got[j] = lax.ppermute(held, ("row", "col"), moves)
        fetched.append(got)
        across = [(i, i ^ 1) for i in range(cols)]
        for j in range(1, half_common + 1):
            got[j], meta = lax.optimization_barrier((got[j], meta))
        swapped.append([lax.ppermute(got[j], "col", across) for j in range(1, half_common + 1)])
    panels = []
    for slot in range(2):
        panels += fetched[slot] + swapped[slot]
    any_space = pl.BlockSpec(memory_space=pl.ANY)
    return pl.pallas_call(
        multiply_kernel,
        out_shape=jax.ShapeDtypeStruct((WB * edge, 2 * WB * edge), jnp.bfloat16),
        in_specs=[pl.BlockSpec(memory_space=pltpu.SMEM)] + [any_space] * (steps + 1 + lists),
        out_specs=any_space,
        scratch_shapes=[
            pltpu.VMEM(((steps + 1) * cap, edge, edge), jnp.bfloat16),
            pltpu.VMEM((lists * cap, edge, edge), jnp.bfloat16),
            pltpu.VMEM((2 * WB * WB + 1, edge, edge), jnp.float32),
            pltpu.VMEM((WB * edge, 2 * WB * edge), jnp.bfloat16),
            pltpu.SemaphoreType.DMA((steps + 1,)),
            pltpu.SemaphoreType.DMA((lists,)),
            pltpu.SemaphoreType.DMA((WB,)),
        ],
        compiler_params=pltpu.CompilerParams(vmem_limit_bytes=48 * 1024 * 1024),
        name="pair_products",
    )(meta, *a_panels, *panels)


def solution(mesh):
    in_specs = (
        P("col", "row", None, None, None),
        P("col", "row", None),
        P("col", "row", None, None, None),
        P("col", "row", None),
        P("col", "row", None, None, None),
        P("col", "row", None),
    )
    out_specs = P("col", "row")
    return jax.shard_map(body, mesh=mesh, in_specs=in_specs, out_specs=out_specs, check_vma=False)
```

```python
import jax
import jax.numpy as jnp
from jax import lax
from jax.experimental import pallas as pl
from jax.experimental.pallas import tpu as pltpu
from jax.sharding import PartitionSpec as P

WB = 10
GROUP = 8


def multiply_kernel(meta, *refs):
    cap, edge = refs[0].shape[0], refs[0].shape[-1]
    out, a_buf, b_buf, acc, stage, a_sems, b_sems, out_sems = refs[-8:]
    wanted_count = a_buf.shape[0] // cap
    a_panels, b_panels = refs[:wanted_count], refs[wanted_count:-8]
    lists = len(b_panels)

    def a_copy(w):
        return pltpu.make_async_copy(a_panels[w], a_buf.at[pl.ds(w * cap, cap)], a_sems.at[w])

    def b_copy(n):
        return pltpu.make_async_copy(b_panels[n], b_buf.at[pl.ds(n * cap, cap)], b_sems.at[n])

    for w in range(wanted_count):
        a_copy(w).start()
    for n in range(lists):
        b_copy(n).start()

    def clear(t, carry):
        acc[t] = jnp.zeros((edge, edge), jnp.float32)
        return carry

    lax.fori_loop(0, acc.shape[0], clear, 0)
    for w in range(wanted_count):
        a_copy(w).wait()
    for n in range(lists):
        b_copy(n).wait()

        def group(g, carry, n=n):
            products = []
            targets = []
            for u in range(GROUP):
                j = g * GROUP + u
                lhs = a_buf[meta[n, j]]
                rhs = b_buf[meta[lists + n, j]]
                targets.append(meta[2 * lists + n, j])
                products.append(jnp.dot(lhs, rhs, preferred_element_type=jnp.float32))
            for u in range(GROUP):
                acc[targets[u]] = acc[targets[u]] + products[u]
            return carry

        lax.fori_loop(0, pl.cdiv(meta[3 * lists, n], GROUP), group, 0)

    def out_copy(r):
        rows = pl.ds(r * edge, edge)
        return pltpu.make_async_copy(stage.at[rows], out.at[rows], out_sems.at[r])

    def finish(r, carry):
        for half in range(2):
            for c in range(WB):
                block = acc[half * WB * WB + r * WB + c].astype(jnp.bfloat16)
                stage[pl.ds(r * edge, edge), (half * WB + c) * edge : (half * WB + c + 1) * edge] = block
        out_copy(r).start()
        return carry

    lax.fori_loop(0, WB, finish, 0)
    for r in range(WB):
        out_copy(r).wait()


def body(a_blocks, a_index, b_blocks, b_index, pair_list, pair_count):
    cap, edge = a_blocks.shape[2], a_blocks.shape[-1]
    steps, pair_cap = pair_list.shape[2], pair_list.shape[-1]
    cols, rows = lax.axis_size("col"), lax.axis_size("row")
    column = lax.axis_index("col")
    row_index = lax.axis_index("row")
    core = column % 2
    half_common = (steps - 1) // 2
    hop = steps // 2 * 2
    ordered = (
        lax.dynamic_index_in_dim(a_blocks[0], core, 0, False),
        lax.dynamic_index_in_dim(a_blocks[0], 1 - core, 0, False),
    )
    first_a, second_a = [], []
    for w in range(hop):
        moves = []
        for i in range(cols):
            for r in range(rows):
                far = w if 2 * i < cols else w + hop
                moves.append(((i + 2 * r + far) % cols // 2 * cols + i, r * cols + i))
        first_a.append(lax.ppermute(ordered[w % 2], ("row", "col"), moves))
    for w in range(hop):
        moves = []
        for i in range(cols):
            for r in range(rows):
                source = (r + (1 if 2 * i < cols else -1) * (hop // 2)) % rows
                moves.append((source * cols + i, r * cols + i))
        second_a.append(lax.ppermute(first_a[w], ("row", "col"), moves))
    a_panels = first_a + second_a

    ids = jnp.concatenate([a_index[0], b_index[0]], axis=-1)
    all_ids = lax.all_gather(ids, ("row", "col"), axis=0).reshape(rows, cols, 2, 2, cap)
    all_ids = all_ids.transpose(1, 0, 2, 3, 4).reshape(cols, 2 * rows, 2, cap)

    pairs = jnp.where(core == 0, pair_list[0], pair_list[0][:, ::-1])
    counts = jnp.where(core == 0, pair_count[0], pair_count[0][:, ::-1])
    place = jnp.arange(steps)
    step = jnp.where(core == 0, place, steps - 1 - place)
    half = jnp.arange(2)
    inner = (column + 2 * row_index + half[:, None] + step[None, :]) % cols
    a_slots, b_slots = pairs[:, :, 0], pairs[:, :, 1]
    a_ids = all_ids[column][inner][:, :, 0]
    b_ids = all_ids[inner, 2 * row_index + half[:, None]][:, :, 1]
    a_at = jnp.take_along_axis(a_ids, a_slots, axis=-1) % WB
    b_at = jnp.take_along_axis(b_ids, b_slots, axis=-1) % WB
    live = jnp.arange(pair_cap) < counts[:, :, None]
    target = jnp.where(live, half[:, None, None] * (WB * WB) + a_at * WB + b_at, 2 * WB * WB)
    a_place = (half[:, None] + step[None, :] + jnp.where(2 * column < cols, 0, hop)) % (2 * hop)
    a_slots = a_slots + a_place[:, :, None] * cap
    b_slots = b_slots + (half[:, None] * steps + place[None, :])[:, :, None] * cap
    lists = 2 * steps
    padded = -(-max(pair_cap, lists) // GROUP) * GROUP

    def laid(x, fill=0):
        x = x.reshape(-1, x.shape[-1]).astype(jnp.int32)
        return jnp.pad(x, ((0, 0), (0, padded - x.shape[1])), constant_values=fill)

    meta = jnp.concatenate(
        [laid(a_slots), laid(b_slots), laid(target, 2 * WB * WB), laid(counts.reshape(1, lists))]
    )

    fetched, swapped = [], []
    for slot in range(2):
        shared = list(range(slot + 1, slot + steps))
        offsets = (
            [slot] + shared[:half_common],
            [slot + steps] + shared[half_common:][::-1],
        )
        got = [None] * (half_common + 1)
        held = b_blocks[0, slot]
        for j in list(range(1, half_common + 1)) + [0]:
            moves = []
            for i in range(cols):
                for r in range(rows):
                    source = (i // 2 * 2 + 2 * r + offsets[i % 2][j]) % cols
                    moves.append((r * cols + source, r * cols + i))
            got[j] = lax.ppermute(held, ("row", "col"), moves)
        fetched.append(got)
        across = [(i, i ^ 1) for i in range(cols)]
        for j in range(1, half_common + 1):
            got[j], meta = lax.optimization_barrier((got[j], meta))
        swapped.append([lax.ppermute(got[j], "col", across) for j in range(1, half_common + 1)])
    panels = []
    for slot in range(2):
        panels += fetched[slot] + swapped[slot]
    any_space = pl.BlockSpec(memory_space=pl.ANY)
    return pl.pallas_call(
        multiply_kernel,
        out_shape=jax.ShapeDtypeStruct((WB * edge, 2 * WB * edge), jnp.bfloat16),
        in_specs=[pl.BlockSpec(memory_space=pltpu.SMEM)] + [any_space] * (steps + 1 + lists),
        out_specs=any_space,
        scratch_shapes=[
            pltpu.VMEM(((steps + 1) * cap, edge, edge), jnp.bfloat16),
            pltpu.VMEM((lists * cap, edge, edge), jnp.bfloat16),
            pltpu.VMEM((2 * WB * WB + 1, edge, edge), jnp.float32),
            pltpu.VMEM((WB * edge, 2 * WB * edge), jnp.bfloat16),
            pltpu.SemaphoreType.DMA((steps + 1,)),
            pltpu.SemaphoreType.DMA((lists,)),
            pltpu.SemaphoreType.DMA((WB,)),
        ],
        compiler_params=pltpu.CompilerParams(vmem_limit_bytes=48 * 1024 * 1024),
        name="pair_products",
    )(meta, *a_panels, *panels)


def solution(mesh):
    in_specs = (
        P("col", "row", None, None, None),
        P("col", "row", None),
        P("col", "row", None, None, None),
        P("col", "row", None),
        P("col", "row", None, None, None),
        P("col", "row", None),
    )
    out_specs = P("col", "row")
    return jax.shard_map(body, mesh=mesh, in_specs=in_specs, out_specs=out_specs, check_vma=False)
```
